768 devices in a mesh: blk: 96 (over x, y_lo, z), rep: 8 (over y_hi, core).
Axes of the slice: x: 4, y: 8 (y_hi: 4, y_lo: 2; y = y_hi * 2 + y_lo), z: 12, core: 2. Of those that a mesh axis runs over, the one named last changes fastest.
Arguments:
- orbitals: bfloat16 [384, 32, 48, 128], P('blk'), may hold values from -6 to 6
- skew: int32 [8], P('rep'), may hold values from 0 to 95
Outputs:
- exchange_fields: float32 [384, 32, 48, 128], P('blk', 'rep')
The draws below stay inside these ranges and needn't reach their ends.
All inputs are finite; a program needn't handle non-finite values.
Results may differ from the reference program's by a relative error of at most 0.0041.
Values may be sent and summed in bfloat16 or wider, within the bound.
No kernel may reach another device: no remote copies, remote signals or barrier semaphores. Data moves between devices by JAX's collectives and lax.ppermute only.
A program may use at most 64 MiB of HBM per device.

```python
import math
import jax
import jax.numpy as jnp
from jax import lax

NX = 32
NY = 48
NZ = 128
ORB_DEV = 4
HOPS = 4
ORBITALS = 384
N_BLK = 96
N_REP = 8


def plant(drawn, stream_key, least, high):
    spot = [jax.random.randint(jax.random.fold_in(stream_key, axis), (), 0, length) for axis, length in enumerate(drawn.shape)]
    longest = drawn.shape.index(max(drawn.shape))
    beside = spot[:longest] + [(spot[longest] + 1) % drawn.shape[longest]] + spot[longest + 1:]
    return drawn.at[tuple(spot)].set(least).at[tuple(beside)].set(high)


def block_scale(rng, extent, pieces, low, high):
    def one(axis_at, shards_of):
        steps = jax.random.uniform(jax.random.fold_in(jax.random.fold_in(rng, 6), axis_at), (shards_of,), jnp.float32, low / len(pieces), high / len(pieces))
        return jnp.repeat(jnp.exp(steps), extent[axis_at] // shards_of).reshape((-1,) + (1,) * (len(extent) - axis_at - 1))

    level = one(*pieces[0])
    for cut in pieces[1:]:
        level = level * one(*cut)
    return level


def noise(key, extent, width, bound, pieces=(), kind=jnp.bfloat16):
    values = jax.random.normal(key, extent, jnp.float32) * width
    if len(pieces) > 0:
        values = block_scale(key, extent, pieces, -0.22, 0.18) * values
    return jnp.clip(values, min=-bound, max=bound).astype(kind)


def setup_inputs(seed: int = 0) -> dict:
    arg_keys = jax.random.split(jax.random.key(seed), 3)
    return {
        "orbitals": noise(arg_keys[0], (ORBITALS, NX, NY, NZ), 1.0, 6.0, ((0, 96),)),
        "skew": plant(jax.random.randint(arg_keys[1], (N_REP,), 0, N_BLK), jax.random.fold_in(arg_keys[1], 1), 0, N_BLK - 1).astype(jnp.int32),
    }


def cas_table(length):
    indices = jnp.arange(length, dtype=jnp.int32)
    products = (indices[:, None] * indices[None, :]) % length
    angles = (2.0 * math.pi / length) * products.astype(jnp.float32)
    return (jnp.cos(angles) + jnp.sin(angles)).astype(jnp.bfloat16)


def frequency_squares(length):
    indices = jnp.arange(length, dtype=jnp.int32)
    signed = jnp.where(indices > length // 2, indices - length, indices)
    wave = (2.0 * math.pi / length) * signed.astype(jnp.float32)
    return wave * wave


def kernel_table():
    squares = frequency_squares(NX)[:, None, None] + frequency_squares(NY)[None, :, None] + frequency_squares(NZ)[None, None, :]
    safe_sq = jnp.where(squares > 0, squares, 1.0)
    kernel = jnp.where(squares > 0, 4.0 * math.pi * (1.0 - jnp.exp(-squares)) / safe_sq, 4.0 * math.pi)
    return kernel / (NX * NY * NZ)


def transform(field, table_x, table_y, table_z):
    first = jnp.einsum('oxyz,zk->oxyk', field.astype(jnp.float32), table_z.astype(jnp.float32)).astype(jnp.bfloat16)
    second = jnp.einsum('oxyz,yk->oxkz', first.astype(jnp.float32), table_y.astype(jnp.float32)).astype(jnp.bfloat16)
    return jnp.einsum('oxyz,xk->okyz', second.astype(jnp.float32), table_x.astype(jnp.float32))


def pair_field(residents, visitor, table_x, table_y, table_z, kernel):
    density = (residents.astype(jnp.float32) * visitor.astype(jnp.float32)[None]).astype(jnp.bfloat16)
    forward = transform(density, table_x, table_y, table_z).astype(jnp.bfloat16)
    scaled = (kernel[None] * forward.astype(jnp.float32)).astype(jnp.bfloat16)
    potential = transform(scaled, table_x, table_y, table_z)
    return potential * visitor.astype(jnp.float32)[None]


def reference(orbitals, skew):
    table_x = cas_table(NX)
    table_y = cas_table(NY)
    table_z = cas_table(NZ)
    kernel = kernel_table()
    owned = orbitals.reshape(N_BLK, ORB_DEV, NX, NY, NZ)
    combos = jnp.arange(N_REP * HOPS, dtype=jnp.int32)
    pairs = jnp.stack([combos // HOPS, combos % HOPS], axis=1)

    def owner_field(owner):
        residents = lax.dynamic_index_in_dim(owned, owner, 0, keepdims=False)

        def advance(field_sum, pair):
            replica = pair[0]
            hop_index = pair[1]
            source = (owner - skew[replica] - hop_index) % N_BLK
            which = (source * ORB_DEV + replica % ORB_DEV).astype(jnp.int32)
            visitor = lax.dynamic_index_in_dim(orbitals, which, 0, keepdims=False)
            return field_sum + pair_field(residents, visitor, table_x, table_y, table_z, kernel), None

        start = jnp.zeros((ORB_DEV, NX, NY, NZ), jnp.float32)
        field_sum, _ = lax.scan(advance, start, pairs)
        return field_sum

    fields = lax.map(owner_field, jnp.arange(N_BLK, dtype=jnp.int32))
    return fields.reshape(ORBITALS, NX, NY, NZ)
```

```python
import functools
import math

import jax
import jax.numpy as jnp
import numpy as np
from jax import lax
from jax.experimental import pallas as pl
from jax.experimental.pallas import tpu as pltpu
from jax.sharding import PartitionSpec as P

NX = 32
NY = 48
NZ = 128
HX = NX // 2
RING = 12
GROUP = 4
ROWS = 16


def cas(rows, cols, length):
    products = np.asarray(rows)[:, None] * np.asarray(cols)[None, :] % length
    angles = np.float32(2.0 * math.pi / length) * products.astype(np.float32)
    return (np.cos(angles) + np.sin(angles)).astype(np.float32)


def frequency_squares(length):
    indices = np.arange(length)
    signed = np.where(indices > length // 2, indices - length, indices)
    wave = np.float32(2.0 * math.pi / length) * signed.astype(np.float32)
    return wave * wave


def kernel_table():
    squares = (
        frequency_squares(NX)[:, None, None]
        + frequency_squares(NY)[None, :, None]
        + frequency_squares(NZ)[None, None, :]
    )
    safe_sq = np.where(squares > 0, squares, np.float32(1.0))
    full = np.float32(4.0 * math.pi)
    kernel = np.where(squares > 0, full * (1.0 - np.exp(-squares)) / safe_sq, full)
    return (kernel / np.float32(NX * NY * NZ)).astype(np.float32)


def tables():
    z_table = np.kron(np.eye(2, dtype=np.float32), cas(range(NZ), range(NZ), NZ))
    y_table = cas(range(NY), range(NY), NY)
    lanes = np.eye(ROWS, dtype=np.float32)
    even = np.kron(cas(range(0, NX, 2), range(HX), NX), lanes)
    odd = np.kron(cas(range(1, NX, 2), range(HX), NX), lanes)
    x_forward = np.stack([even, odd])
    x_back = np.stack([even.T, odd.T])
    kernel = kernel_table().reshape(HX, 2, NY // ROWS, ROWS, NZ).transpose(1, 2, 0, 3, 4)
    kernel = kernel.reshape(2, NY // ROWS, HX * ROWS, NZ)
    return tuple(jnp.asarray(t, jnp.bfloat16) for t in (z_table, y_table, x_forward, x_back)) + (
        jnp.asarray(kernel),
    )


def pair_kernel(has_sum, *refs):
    if has_sum:
        orb, vis, acc, z_table, y_table, x_forward, x_back, kernel, out, waves, points = refs
    else:
        orb, vis, z_table, y_table, x_forward, x_back, kernel, out, waves, points = refs
    dot = functools.partial(jnp.dot, preferred_element_type=jnp.float32)
    bf16 = jnp.bfloat16

    def forward(group, _):
        rows = []
        for i in range(GROUP):
            x = group * GROUP + i
            for o in range(2):
                rows.append(
                    jnp.concatenate([orb[o, x] * vis[x], orb[o, x + HX] * vis[x + HX]], axis=1)
                )
        a = dot(jnp.concatenate(rows, axis=0), z_table[...]).astype(bf16)
        a = jnp.concatenate([a[j * NY : (j + 1) * NY] for j in range(2 * GROUP)], axis=1)
        b = dot(y_table[...], a)
        for i in range(GROUP):
            for o in range(2):
                at = (i * 2 + o) * 2 * NZ
                low, high = b[:, at : at + NZ], b[:, at + NZ : at + 2 * NZ]
                for parity, t in enumerate((low + high, low - high)):
                    t = t.astype(bf16)
                    for part in range(NY // ROWS):
                        waves[parity, part, group * GROUP + i, :, o * NZ : (o + 1) * NZ] = t[
                            part * ROWS : (part + 1) * ROWS
                        ]
        return 0

    lax.fori_loop(0, HX // GROUP, forward, 0)
    for part in range(NY // ROWS):
        halves = []
        for parity in range(2):
            m = dot(x_forward[parity], waves[parity, part].reshape(HX * ROWS, 2 * NZ))
            k = kernel[parity, part]
            m = (m * jnp.concatenate([k, k], axis=1)).astype(bf16)
            halves.append(dot(x_back[parity], m))
        for h, t in enumerate((halves[0] + halves[1], halves[0] - halves[1])):
            points[:, h, part * ROWS : (part + 1) * ROWS, :] = t.astype(bf16).reshape(
                HX, ROWS, 2 * NZ
            )

    def backward(group, _):
        b = jnp.concatenate(
            [
                points[group * GROUP + i, h, :, o * NZ : (o + 1) * NZ]
                for i in range(GROUP)
                for o in range(2)
                for h in range(2)
            ],
            axis=1,
        )
        b = dot(y_table[...], b).astype(bf16)
        a = jnp.concatenate(
            [b[:, j * 2 * NZ : (j + 1) * 2 * NZ] for j in range(2 * GROUP)], axis=0
        )
        c = dot(a, z_table[...])
        for i in range(GROUP):
            for o in range(2):
                at = (i * 2 + o) * NY
                for h in range(2):
                    x = group * GROUP + i + h * HX
                    t = c[at : at + NY, h * NZ : (h + 1) * NZ] * vis[x].astype(jnp.float32)
                    out[o, x] = t + acc[o, x] if has_sum else t
        return 0

    lax.fori_loop(0, HX // GROUP, backward, 0)


def add_pairs(orbitals, visitor, field_sum, constants):
    count = orbitals.shape[0]

    def whole(value):
        return pl.BlockSpec(value.shape, lambda i, nd=value.ndim: (0,) * nd)

    block = pl.BlockSpec((2, NX, NY, NZ), lambda i: (i, 0, 0, 0))
    sums = [] if field_sum is None else [field_sum]
    return pl.pallas_call(
        functools.partial(pair_kernel, field_sum is not None),
        out_shape=jax.ShapeDtypeStruct((count, NX, NY, NZ), jnp.float32),
        grid=(count // 2,),
        in_specs=[block, whole(visitor)] + [block for _ in sums] + [whole(t) for t in constants],
        out_specs=block,
        scratch_shapes=[
            pltpu.VMEM((2, NY // ROWS, HX, ROWS, 2 * NZ), jnp.bfloat16),
            pltpu.VMEM((HX, 2, NY, 2 * NZ), jnp.bfloat16),
        ],
        input_output_aliases={2: 0} if sums else {},
        compiler_params=pltpu.CompilerParams(vmem_limit_bytes=40 * 2**20),
        cost_estimate=pl.CostEstimate(
            flops=8_000_000_000, bytes_accessed=8 * 2**20, transcendentals=0
        ),
        name="pair_field",
    )(orbitals, visitor, *sums, *constants)


def shifted(value, axis, steps):
    count = lax.axis_size(axis)
    return lax.ppermute(value, axis, [(i, (i + steps) % count) for i in range(count)])


def shift_by(visitor, offset):
    rings = lax.axis_size("blk") // RING
    within = offset % RING
    whole = (offset // RING + jnp.where(within > RING // 2, 1, 0)) % rings

    def mover(steps):
        return (lambda v: shifted(v, "blk", steps)) if steps else (lambda v: v)

    visitor = lax.switch(whole, [mover(RING * j) for j in range(rings)], visitor)
    near = [j if j <= RING // 2 else j - RING for j in range(RING)]
    return lax.switch(within, [mover(j) for j in near], visitor)


def spread(field_sum):
    replica = lax.axis_index("rep")
    chips = lax.axis_size("rep") // 2
    core, chip = replica % 2, replica // 2
    count = field_sum.shape[0]
    parts = field_sum.reshape(count, chips, 2, NX // (2 * chips), NY, NZ)
    sent = lax.dynamic_index_in_dim(parts, 1 - core, 2, keepdims=False).astype(jnp.bfloat16)
    other = lax.ppermute(sent, "rep", [(i, i ^ 1) for i in range(2 * chips)])
    mine = lax.dynamic_index_in_dim(parts, core, 2, keepdims=False) + other.astype(jnp.float32)
    total = lax.dynamic_index_in_dim(mine, chip, 1, keepdims=False)
    short = mine.astype(jnp.bfloat16)
    for step in (2, 1, 3):
        part = lax.dynamic_index_in_dim(short, (chip + step) % chips, 1, keepdims=False)
        total = total + shifted(part, "rep", 2 * step).astype(jnp.float32)
    return total


def body(orbitals, skew):
    constants = tables()
    replica = lax.axis_index("rep")
    start_orb = lax.dynamic_index_in_dim(orbitals, replica % orbitals.shape[0], 0, keepdims=False)
    second = shift_by(start_orb, (skew[0] + 1) % lax.axis_size("blk"))
    third = shifted(second, "blk", 1)
    first = shifted(second, "blk", -1)
    field_sum = add_pairs(orbitals, second, None, constants)
    fourth = shifted(third, "blk", 1)
    field_sum = add_pairs(orbitals, third, field_sum, constants)
    field_sum = add_pairs(orbitals, first, field_sum, constants)
    field_sum = add_pairs(orbitals, fourth, field_sum, constants)
    return spread(field_sum)


def solution(mesh):
    placed = (P("blk", None, None, None), P("rep"))
    return jax.shard_map(
        body, mesh=mesh, in_specs=placed, out_specs=P("blk", "rep", None, None), check_vma=False
    )
```

```python
import functools
import math

import jax
import jax.numpy as jnp
import numpy as np
from jax import lax
from jax.experimental import pallas as pl
from jax.experimental.pallas import tpu as pltpu
from jax.sharding import PartitionSpec as P

NX = 32
NY = 48
NZ = 128
HX = NX // 2
RING = 12
GROUP = 16
HOPS = 4
ROWS = 16


def cas(rows, cols, length):
    products = np.asarray(rows)[:, None] * np.asarray(cols)[None, :] % length
    angles = np.float32(2.0 * math.pi / length) * products.astype(np.float32)
    return (np.cos(angles) + np.sin(angles)).astype(np.float32)


def frequency_squares(length):
    indices = np.arange(length)
    signed = np.where(indices > length // 2, indices - length, indices)
    wave = np.float32(2.0 * math.pi / length) * signed.astype(np.float32)
    return wave * wave


def kernel_table():
    squares = (
        frequency_squares(NX)[:, None, None]
        + frequency_squares(NY)[None, :, None]
        + frequency_squares(NZ)[None, None, :]
    )
    safe_sq = np.where(squares > 0, squares, np.float32(1.0))
    full = np.float32(4.0 * math.pi)
    kernel = np.where(squares > 0, full * (1.0 - np.exp(-squares)) / safe_sq, full)
    return (kernel / np.float32(NX * NY * NZ)).astype(np.float32)


def tables():
    z_table = np.kron(np.eye(2, dtype=np.float32), cas(range(NZ), range(NZ), NZ))
    y_table = cas(range(NY), range(NY), NY)
    lanes = np.eye(ROWS, dtype=np.float32)
    even = np.kron(cas(range(0, NX, 2), range(HX), NX), lanes)
    odd = np.kron(cas(range(1, NX, 2), range(HX), NX), lanes)
    kernel = kernel_table().reshape(HX, 2, NY // ROWS, ROWS, NZ).transpose(1, 2, 0, 3, 4)
    kernel = kernel.reshape(2, NY // ROWS, HX * ROWS, NZ)
    y_table = np.pad(y_table, ((0, 0), (0, 2 * NZ - NY)))
    table = np.concatenate([z_table, even, odd, even.T, odd.T, y_table])
    return jnp.asarray(table, jnp.bfloat16), jnp.asarray(kernel)


def pair_kernel(has_sum, *refs):
    if has_sum:
        orb, vis, acc, table, kernel, out, waves, points = refs
    else:
        orb, vis, table, kernel, out, waves, points = refs
    dot = functools.partial(jnp.dot, preferred_element_type=jnp.float32)
    bf16 = jnp.bfloat16
    z_table, *x_tables = (table.at[pl.ds(i * 256, 256)] for i in range(5))
    x_forward, x_back = x_tables[:2], x_tables[2:]
    y_table = table[5 * 256 :, :NY]

    def forward(group, _):
        rows = []
        for i in range(GROUP):
            x = group * GROUP + i
            for o in range(2):
                rows.append(
                    jnp.concatenate([orb[o, x] * vis[x], orb[o, x + HX] * vis[x + HX]], axis=1)
                )
        a = dot(jnp.concatenate(rows, axis=0), z_table[...]).astype(bf16)
        a = jnp.concatenate([a[j * NY : (j + 1) * NY] for j in range(2 * GROUP)], axis=1)
        b = dot(y_table, a)
        for i in range(GROUP):
            for o in range(2):
                at = (i * 2 + o) * 2 * NZ
                low, high = b[:, at : at + NZ], b[:, at + NZ : at + 2 * NZ]
                for parity, t in enumerate((low + high, low - high)):
                    t = t.astype(bf16)
                    for part in range(NY // ROWS):
                        waves[parity, part, group * GROUP + i, :, o * NZ : (o + 1) * NZ] = t[
                            part * ROWS : (part + 1) * ROWS
                        ]
        return 0

    lax.fori_loop(0, HX // GROUP, forward, 0)
    for part in range(NY // ROWS):
        halves = []
        for parity in range(2):
            m = dot(x_forward[parity][...], waves[parity, part].reshape(HX * ROWS, 2 * NZ))
            k = kernel[parity, part]
            m = (m * jnp.concatenate([k, k], axis=1)).astype(bf16)
            halves.append(dot(x_back[parity][...], m))
        for h, t in enumerate((halves[0] + halves[1], halves[0] - halves[1])):
            points[:, h, part * ROWS : (part + 1) * ROWS, :] = t.astype(bf16).reshape(
                HX, ROWS, 2 * NZ
            )

    def backward(group, _):
        b = jnp.concatenate(
            [
                points[group * GROUP + i, h, :, o * NZ : (o + 1) * NZ]
                for i in range(GROUP)
                for o in range(2)
                for h in range(2)
            ],
            axis=1,
        )
        b = dot(y_table, b).astype(bf16)
        a = jnp.concatenate(
            [b[:, j * 2 * NZ : (j + 1) * 2 * NZ] for j in range(2 * GROUP)], axis=0
        )
        c = dot(a, z_table[...])
        for i in range(GROUP):
            for o in range(2):
                at = (i * 2 + o) * NY
                for h in range(2):
                    x = group * GROUP + i + h * HX
                    t = c[at : at + NY, h * NZ : (h + 1) * NZ] * vis[x].astype(jnp.float32)
                    out[o, x] = t + acc[o, x] if has_sum else t
        return 0

    lax.fori_loop(0, HX // GROUP, backward, 0)


def add_pairs(orbitals, visitor, field_sum, constants):
    count = orbitals.shape[0]

    def whole(value):
        return pl.BlockSpec(value.shape, lambda i, nd=value.ndim: (0,) * nd)

    block = pl.BlockSpec((2, NX, NY, NZ), lambda i: (i, 0, 0, 0))
    sums = [] if field_sum is None else [field_sum]
    return pl.pallas_call(
        functools.partial(pair_kernel, field_sum is not None),
        out_shape=jax.ShapeDtypeStruct((count, NX, NY, NZ), jnp.float32),
        grid=(count // 2,),
        in_specs=[block, whole(visitor)] + [block for _ in sums] + [whole(t) for t in constants],
        out_specs=block,
        scratch_shapes=[
            pltpu.VMEM((2, NY // ROWS, HX, ROWS, 2 * NZ), jnp.bfloat16),
            pltpu.VMEM((HX, 2, NY, 2 * NZ), jnp.bfloat16),
        ],
        input_output_aliases={2: 0} if sums else {},
        compiler_params=pltpu.CompilerParams(vmem_limit_bytes=24 * 2**20),
        cost_estimate=pl.CostEstimate(
            flops=8_000_000_000, bytes_accessed=8 * 2**20, transcendentals=0
        ),
        name="pair_field",
    )(orbitals, visitor, *sums, *constants)


def shifted(value, axis, steps):
    count = lax.axis_size(axis)
    return lax.ppermute(value, axis, [(i, (i + steps) % count) for i in range(count)])


def shift_by(visitor, offset):
    rings = lax.axis_size("blk") // RING
    within = offset % RING
    whole = (offset // RING + jnp.where(within > RING // 2, 1, 0)) % rings

    def mover(steps):
        return (lambda v: shifted(v, "blk", steps)) if steps else (lambda v: v)

    visitor = lax.switch(whole, [mover(RING * j) for j in range(rings)], visitor)
    near = [j if j <= RING // 2 else j - RING for j in range(RING)]
    return lax.switch(within, [mover(j) for j in near], visitor)


def paired(value, even, odd):
    count = lax.axis_size("rep")
    pairs = [(i, (i + (odd if i % 2 else even)) % count) for i in range(count)]
    return lax.ppermute(value, "rep", pairs)


def merge_kernel(place, parts, other, kept, ahead_rows, far, back):
    core, chip, ahead, behind, across = (place[i] for i in range(5))
    for target, at in ((far, across), (back, behind), (kept, chip), (ahead_rows, ahead)):
        for o in range(parts.shape[0]):
            for x in range(parts.shape[3]):
                t = parts[o, at, core, x] + other[o, at, x].astype(jnp.float32)
                target[o, x] = t.astype(target.dtype)


def merge(place, parts, other):
    count, _, _, rows = parts.shape[:4]
    shape = (count, rows, NY, NZ)
    kinds = (jnp.float32, jnp.float32, jnp.bfloat16, jnp.bfloat16)
    space = pl.BlockSpec(memory_space=pltpu.VMEM)
    return pl.pallas_call(
        merge_kernel,
        out_shape=[jax.ShapeDtypeStruct(shape, kind) for kind in kinds],
        grid_spec=pltpu.PrefetchScalarGridSpec(
            num_scalar_prefetch=1, grid=(), in_specs=[space] * 2, out_specs=[space] * 4
        ),
        compiler_params=pltpu.CompilerParams(vmem_limit_bytes=16 * 2**20),
        name="merge",
    )(place, parts, other)


def spread(field_sum):
    replica = lax.axis_index("rep")
    chips = lax.axis_size("rep") // 2
    core, chip = replica % 2, replica // 2
    ahead = jnp.where(core == 0, chip + 1, chip + chips - 1) % chips
    across = (chip + 2) % chips
    behind = (ahead + 2) % chips
    count = field_sum.shape[0]
    parts = field_sum.reshape(count, chips, 2, NX // (2 * chips), NY, NZ)
    sent = lax.dynamic_index_in_dim(parts, 1 - core, 2, keepdims=False).astype(jnp.bfloat16)
    other = paired(sent, 1, -1)
    place = jnp.stack([core, chip, ahead, behind, across]).astype(jnp.int32)
    kept, ahead_rows, far, back = merge(place, parts, other)
    far = paired(far, 2, -2)
    back = paired(back, -2, 2)
    near = paired((ahead_rows + far.astype(jnp.float32)).astype(jnp.bfloat16), 2, -2)
    return kept + back.astype(jnp.float32) + near.astype(jnp.float32)


def hop(visitor):
    owners, replicas = lax.axis_size("blk"), lax.axis_size("rep")
    pairs = [
        (b * replicas + r, (b + (-1 if r % 2 else 1)) % owners * replicas + r)
        for b in range(owners)
        for r in range(replicas)
    ]
    return lax.ppermute(visitor, ("blk", "rep"), pairs)


def body(orbitals, skew):
    constants = tables()
    replica = lax.axis_index("rep")
    start_orb = lax.dynamic_index_in_dim(orbitals, replica % orbitals.shape[0], 0, keepdims=False)
    first = skew[0] + jnp.where(replica % 2 == 0, 0, HOPS - 1)
    visitor = shift_by(start_orb, first % lax.axis_size("blk"))
    field_sum = None
    for hop_index in range(HOPS):
        following = hop(visitor) if hop_index < HOPS - 1 else None
        field_sum = add_pairs(orbitals, visitor, field_sum, constants)
        visitor = following
    return spread(field_sum)


def solution(mesh):
    placed = (P("blk", None, None, None), P("rep"))
    return jax.shard_map(
        body, mesh=mesh, in_specs=placed, out_specs=P("blk", "rep", None, None), check_vma=False
    )
```

```python
import functools
import math

import jax
import jax.numpy as jnp
import numpy as np
from jax import lax
from jax.experimental import pallas as pl
from jax.experimental.pallas import tpu as pltpu
from jax.sharding import PartitionSpec as P

NX = 32
NY = 48
NZ = 128
HX = NX // 2
RING = 12
GROUP = 16
HOPS = 4
ROWS = 16


def cas(rows, cols, length):
    products = np.asarray(rows)[:, None] * np.asarray(cols)[None, :] % length
    angles = np.float32(2.0 * math.pi / length) * products.astype(np.float32)
    return (np.cos(angles) + np.sin(angles)).astype(np.float32)


def frequency_squares(length):
    indices = np.arange(length)
    signed = np.where(indices > length // 2, indices - length, indices)
    wave = np.float32(2.0 * math.pi / length) * signed.astype(np.float32)
    return wave * wave


def kernel_table():
    squares = (
        frequency_squares(NX)[:, None, None]
        + frequency_squares(NY)[None, :, None]
        + frequency_squares(NZ)[None, None, :]
    )
    safe_sq = np.where(squares > 0, squares, np.float32(1.0))
    full = np.float32(4.0 * math.pi)
    kernel = np.where(squares > 0, full * (1.0 - np.exp(-squares)) / safe_sq, full)
    return (kernel / np.float32(NX * NY * NZ)).astype(np.float32)


def tables():
    z_table = np.kron(np.eye(2, dtype=np.float32), cas(range(NZ), range(NZ), NZ))
    y_table = cas(range(NY), range(NY), NY)
    lanes = np.eye(ROWS, dtype=np.float32)
    even = np.kron(cas(range(0, NX, 2), range(HX), NX), lanes)
    odd = np.kron(cas(range(1, NX, 2), range(HX), NX), lanes)
    kernel = kernel_table().reshape(HX, 2, NY // ROWS, ROWS, NZ).transpose(1, 2, 0, 3, 4)
    kernel = kernel.reshape(2, NY // ROWS, HX * ROWS, NZ)
    y_table = np.pad(y_table, ((0, 0), (0, 2 * NZ - NY)))
    table = np.concatenate([z_table, even, odd, even.T, odd.T, y_table])
    return jnp.asarray(table, jnp.bfloat16), jnp.asarray(kernel)


def pair_kernel(has_sum, *refs):
    if has_sum:
        orb, vis, acc, table, kernel, out, waves, points = refs
    else:
        orb, vis, table, kernel, out, waves, points = refs
    dot = functools.partial(jnp.dot, preferred_element_type=jnp.float32)
    bf16 = jnp.bfloat16
    z_table, *x_tables = (table.at[pl.ds(i * 256, 256)] for i in range(5))
    x_forward, x_back = x_tables[:2], x_tables[2:]
    y_table = table[5 * 256 :, :NY]

    def forward(group, _):
        rows = []
        for i in range(GROUP):
            x = group * GROUP + i
            for o in range(2):
                rows.append(
                    jnp.concatenate([orb[o, x] * vis[x], orb[o, x + HX] * vis[x + HX]], axis=1)
                )
        a = dot(jnp.concatenate(rows, axis=0), z_table[...]).astype(bf16)
        a = jnp.concatenate([a[j * NY : (j + 1) * NY] for j in range(2 * GROUP)], axis=1)
        b = dot(y_table, a)
        for i in range(GROUP):
            for o in range(2):
                at = (i * 2 + o) * 2 * NZ
                low, high = b[:, at : at + NZ], b[:, at + NZ : at + 2 * NZ]
                for parity, t in enumerate((low + high, low - high)):
                    t = t.astype(bf16)
                    for part in range(NY // ROWS):
                        waves[parity, part, group * GROUP + i, :, o * NZ : (o + 1) * NZ] = t[
                            part * ROWS : (part + 1) * ROWS
                        ]
        return 0

    lax.fori_loop(0, HX // GROUP, forward, 0)
    for part in range(NY // ROWS):
        halves = []
        for parity in range(2):
            m = dot(x_forward[parity][...], waves[parity, part].reshape(HX * ROWS, 2 * NZ))
            k = kernel[parity, part]
            m = (m * jnp.concatenate([k, k], axis=1)).astype(bf16)
            halves.append(dot(x_back[parity][...], m))
        for h, t in enumerate((halves[0] + halves[1], halves[0] - halves[1])):
            points[:, h, part * ROWS : (part + 1) * ROWS, :] = t.astype(bf16).reshape(
                HX, ROWS, 2 * NZ
            )

    def backward(group, _):
        b = jnp.concatenate(
            [
                points[group * GROUP + i, h, :, o * NZ : (o + 1) * NZ]
                for i in range(GROUP)
                for o in range(2)
                for h in range(2)
            ],
            axis=1,
        )
        b = dot(y_table, b).astype(bf16)
        a = jnp.concatenate(
            [b[:, j * 2 * NZ : (j + 1) * 2 * NZ] for j in range(2 * GROUP)], axis=0
        )
        c = dot(a, z_table[...])
        for i in range(GROUP):
            for o in range(2):
                at = (i * 2 + o) * NY
                for h in range(2):
                    x = group * GROUP + i + h * HX
                    t = c[at : at + NY, h * NZ : (h + 1) * NZ] * vis[x].astype(jnp.float32)
                    out[o, x] = t + acc[o, x] if has_sum else t
        return 0

    lax.fori_loop(0, HX // GROUP, backward, 0)


def add_pairs(orbitals, visitor, field_sum, constants):
    count = orbitals.shape[0]

    def whole(value):
        return pl.BlockSpec(value.shape, lambda i, nd=value.ndim: (0,) * nd)

    block = pl.BlockSpec((2, NX, NY, NZ), lambda i: (i, 0, 0, 0))
    sums = [] if field_sum is None else [field_sum]
    return pl.pallas_call(
        functools.partial(pair_kernel, field_sum is not None),
        out_shape=jax.ShapeDtypeStruct((count, NX, NY, NZ), jnp.float32),
        grid=(count // 2,),
        in_specs=[block, whole(visitor)] + [block for _ in sums] + [whole(t) for t in constants],
        out_specs=block,
        scratch_shapes=[
            pltpu.VMEM((2, NY // ROWS, HX, ROWS, 2 * NZ), jnp.bfloat16),
            pltpu.VMEM((HX, 2, NY, 2 * NZ), jnp.bfloat16),
        ],
        input_output_aliases={2: 0} if sums else {},
        compiler_params=pltpu.CompilerParams(vmem_limit_bytes=24 * 2**20),
        cost_estimate=pl.CostEstimate(
            flops=8_000_000_000, bytes_accessed=8 * 2**20, transcendentals=0
        ),
        name="pair_field",
    )(orbitals, visitor, *sums, *constants)


def shifted(value, axis, steps):
    count = lax.axis_size(axis)
    return lax.ppermute(value, axis, [(i, (i + steps) % count) for i in range(count)])


def shift_by(visitor, offset):
    rings = lax.axis_size("blk") // RING
    within = offset % RING
    whole = (offset // RING + jnp.where(within > RING // 2, 1, 0)) % rings

    def mover(steps, pieces=1):
        def move(v):
            cut = v.shape[0] // pieces
            parts = [shifted(v[i * cut : (i + 1) * cut], "blk", steps) for i in range(pieces)]
            return jnp.concatenate(parts) if pieces > 1 else parts[0]

        return move if steps else (lambda v: v)

    visitor = lax.switch(whole, [mover(RING * j) for j in range(rings)], visitor)
    near = [j if j <= RING // 2 else j - RING for j in range(RING)]
    return lax.switch(within, [mover(j, 2 if abs(j) < 4 else 1) for j in near], visitor)


def paired(value, even, odd):
    count = lax.axis_size("rep")
    pairs = [(i, (i + (odd if i % 2 else even)) % count) for i in range(count)]
    return lax.ppermute(value, "rep", pairs)


def merge_kernel(place, parts, other, kept, ahead_rows, far, back):
    core, chip, ahead, behind, across = (place[i] for i in range(5))
    for target, at in ((far, across), (back, behind), (kept, chip), (ahead_rows, ahead)):
        for o in range(parts.shape[0]):
            for x in range(parts.shape[3]):
                t = parts[o, at, core, x] + other[o, at, x].astype(jnp.float32)
                target[o, x] = t.astype(target.dtype)


def merge(place, parts, other):
    count, _, _, rows = parts.shape[:4]
    shape = (count, rows, NY, NZ)
    kinds = (jnp.float32, jnp.float32, jnp.bfloat16, jnp.bfloat16)
    space = pl.BlockSpec(memory_space=pltpu.VMEM)
    return pl.pallas_call(
        merge_kernel,
        out_shape=[jax.ShapeDtypeStruct(shape, kind) for kind in kinds],
        grid_spec=pltpu.PrefetchScalarGridSpec(
            num_scalar_prefetch=1, grid=(), in_specs=[space] * 2, out_specs=[space] * 4
        ),
        compiler_params=pltpu.CompilerParams(vmem_limit_bytes=16 * 2**20),
        name="merge",
    )(place, parts, other)


def spread(field_sum):
    replica = lax.axis_index("rep")
    chips = lax.axis_size("rep") // 2
    core, chip = replica % 2, replica // 2
    ahead = jnp.where(core == 0, chip + 1, chip + chips - 1) % chips
    across = (chip + 2) % chips
    behind = (ahead + 2) % chips
    count = field_sum.shape[0]
    parts = field_sum.reshape(count, chips, 2, NX // (2 * chips), NY, NZ)
    sent = lax.dynamic_index_in_dim(parts, 1 - core, 2, keepdims=False).astype(jnp.bfloat16)
    other = paired(sent, 1, -1)
    place = jnp.stack([core, chip, ahead, behind, across]).astype(jnp.int32)
    kept, ahead_rows, far, back = merge(place, parts, other)
    far = paired(far, 2, -2)
    back = paired(back, -2, 2)
    near = paired((ahead_rows + far.astype(jnp.float32)).astype(jnp.bfloat16), 2, -2)
    return kept + back.astype(jnp.float32) + near.astype(jnp.float32)


def moved(visitor, target):
    owners, replicas = lax.axis_size("blk"), lax.axis_size("rep")
    pairs = []
    for b in range(owners):
        for r in range(replicas):
            steps = target(b % RING, -1 if r % 2 else 1)
            if steps:
                pairs.append((b * replicas + r, (b + steps) % owners * replicas + r))
    return lax.ppermute(visitor, ("blk", "rep"), pairs)


def hop(visitor):
    return moved(visitor, lambda z, way: way if 0 <= z + way < RING else 0)


def carry(visitor, hops):
    return moved(
        visitor, lambda z, way: way * hops if z == (RING - hops if way > 0 else hops - 1) else 0
    )


def body(orbitals, skew):
    constants = tables()
    replica = lax.axis_index("rep")
    start_orb = lax.dynamic_index_in_dim(orbitals, replica % orbitals.shape[0], 0, keepdims=False)
    first = skew[0] + jnp.where(replica % 2 == 0, 0, HOPS - 1)
    visitor = shift_by(start_orb, first % lax.axis_size("blk"))
    place = lax.axis_index("blk") % RING
    edge = place == jnp.where(replica % 2 == 0, 0, RING - 1)
    carried = [carry(visitor, hops) for hops in range(1, HOPS)]
    field_sum = None
    for hop_index in range(HOPS):
        following = None
        if hop_index < HOPS - 1:
            following = jnp.where(edge, carried[hop_index], hop(visitor))
        field_sum = add_pairs(orbitals, visitor, field_sum, constants)
        visitor = following
    return spread(field_sum)


def solution(mesh):
    placed = (P("blk", None, None, None), P("rep"))
    return jax.shard_map(
        body, mesh=mesh, in_specs=placed, out_specs=P("blk", "rep", None, None), check_vma=False
    )
```

```python
import functools
import math

import jax
import jax.numpy as jnp
import numpy as np
from jax import lax
from jax.experimental import pallas as pl
from jax.experimental.pallas import tpu as pltpu
from jax.sharding import PartitionSpec as P

NX = 32
NY = 48
NZ = 128
HX = NX // 2
RING = 12
GROUP = 16
HOPS = 4
ROWS = 16


def cas(rows, cols, length):
    products = np.asarray(rows)[:, None] * np.asarray(cols)[None, :] % length
    angles = np.float32(2.0 * math.pi / length) * products.astype(np.float32)
    return (np.cos(angles) + np.sin(angles)).astype(np.float32)


def frequency_squares(length):
    indices = np.arange(length)
    signed = np.where(indices > length // 2, indices - length, indices)
    wave = np.float32(2.0 * math.pi / length) * signed.astype(np.float32)
    return wave * wave


def kernel_table():
    squares = (
        frequency_squares(NX)[:, None, None]
        + frequency_squares(NY)[None, :, None]
        + frequency_squares(NZ)[None, None, :]
    )
    safe_sq = np.where(squares > 0, squares, np.float32(1.0))
    full = np.float32(4.0 * math.pi)
    kernel = np.where(squares > 0, full * (1.0 - np.exp(-squares)) / safe_sq, full)
    return (kernel / np.float32(NX * NY * NZ)).astype(np.float32)


def tables():
    z_table = np.kron(np.eye(2, dtype=np.float32), cas(range(NZ), range(NZ), NZ))
    y_table = cas(range(NY), range(NY), NY)
    lanes = np.eye(ROWS, dtype=np.float32)
    even = np.kron(cas(range(0, NX, 2), range(HX), NX), lanes)
    odd = np.kron(cas(range(1, NX, 2), range(HX), NX), lanes)
    kernel = kernel_table().reshape(HX, 2, NY // ROWS, ROWS, NZ).transpose(1, 2, 0, 3, 4)
    kernel = kernel.reshape(2, NY // ROWS, HX * ROWS, NZ)
    y_table = np.pad(y_table, ((0, 0), (0, 2 * NZ - NY)))
    table = np.concatenate([z_table, even, odd, even.T, odd.T, y_table])
    return jnp.asarray(table, jnp.bfloat16), jnp.asarray(kernel)


def pair_kernel(has_sum, *refs):
    if has_sum:
        orb, vis, acc, table, kernel, out, waves, points = refs
    else:
        orb, vis, table, kernel, out, waves, points = refs
    dot = functools.partial(jnp.dot, preferred_element_type=jnp.float32)
    bf16 = jnp.bfloat16
    z_table, *x_tables = (table.at[pl.ds(i * 256, 256)] for i in range(5))
    x_forward, x_back = x_tables[:2], x_tables[2:]
    y_table = table[5 * 256 :, :NY]

    def forward(group, _):
        rows = []
        for i in range(GROUP):
            x = group * GROUP + i
            for o in range(2):
                rows.append(
                    jnp.concatenate([orb[o, x] * vis[x], orb[o, x + HX] * vis[x + HX]], axis=1)
                )
        a = dot(jnp.concatenate(rows, axis=0), z_table[...]).astype(bf16)
        a = jnp.concatenate([a[j * NY : (j + 1) * NY] for j in range(2 * GROUP)], axis=1)
        b = dot(y_table, a)
        for i in range(GROUP):
            for o in range(2):
                at = (i * 2 + o) * 2 * NZ
                low, high = b[:, at : at + NZ], b[:, at + NZ : at + 2 * NZ]
                for parity, t in enumerate((low + high, low - high)):
                    t = t.astype(bf16)
                    for part in range(NY // ROWS):
                        waves[parity, part, group * GROUP + i, :, o * NZ : (o + 1) * NZ] = t[
                            part * ROWS : (part + 1) * ROWS
                        ]
        return 0

    lax.fori_loop(0, HX // GROUP, forward, 0)
    for part in range(NY // ROWS):
        halves = []
        for parity in range(2):
            m = dot(x_forward[parity][...], waves[parity, part].reshape(HX * ROWS, 2 * NZ))
            k = kernel[parity, part]
            m = (m * jnp.concatenate([k, k], axis=1)).astype(bf16)
            halves.append(dot(x_back[parity][...], m))
        for h, t in enumerate((halves[0] + halves[1], halves[0] - halves[1])):
            points[:, h, part * ROWS : (part + 1) * ROWS, :] = t.astype(bf16).reshape(
                HX, ROWS, 2 * NZ
            )

    def backward(group, _):
        b = jnp.concatenate(
            [
                points[group * GROUP + i, h, :, o * NZ : (o + 1) * NZ]
                for i in range(GROUP)
                for o in range(2)
                for h in range(2)
            ],
            axis=1,
        )
        b = dot(y_table, b).astype(bf16)
        a = jnp.concatenate(
            [b[:, j * 2 * NZ : (j + 1) * 2 * NZ] for j in range(2 * GROUP)], axis=0
        )
        c = dot(a, z_table[...])
        for i in range(GROUP):
            for o in range(2):
                at = (i * 2 + o) * NY
                for h in range(2):
                    x = group * GROUP + i + h * HX
                    t = c[at : at + NY, h * NZ : (h + 1) * NZ] * vis[x].astype(jnp.float32)
                    out[o, x] = t + acc[o, x] if has_sum else t
        return 0

    lax.fori_loop(0, HX // GROUP, backward, 0)


def add_pairs(orbitals, visitor, field_sum, constants):
    count = orbitals.shape[0]

    def whole(value):
        return pl.BlockSpec(value.shape, lambda i, nd=value.ndim: (0,) * nd)

    block = pl.BlockSpec((2, NX, NY, NZ), lambda i: (i, 0, 0, 0))
    sums = [] if field_sum is None else [field_sum]
    return pl.pallas_call(
        functools.partial(pair_kernel, field_sum is not None),
        out_shape=jax.ShapeDtypeStruct((count, NX, NY, NZ), jnp.float32),
        grid=(count // 2,),
        in_specs=[block, whole(visitor)] + [block for _ in sums] + [whole(t) for t in constants],
        out_specs=block,
        scratch_shapes=[
            pltpu.VMEM((2, NY // ROWS, HX, ROWS, 2 * NZ), jnp.bfloat16),
            pltpu.VMEM((HX, 2, NY, 2 * NZ), jnp.bfloat16),
        ],
        input_output_aliases={2: 0} if sums else {},
        compiler_params=pltpu.CompilerParams(vmem_limit_bytes=24 * 2**20),
        cost_estimate=pl.CostEstimate(
            flops=8_000_000_000, bytes_accessed=8 * 2**20, transcendentals=0
        ),
        name="pair_field",
    )(orbitals, visitor, *sums, *constants)


def shifted(value, axis, steps):
    count = lax.axis_size(axis)
    return lax.ppermute(value, axis, [(i, (i + steps) % count) for i in range(count)])


def shift_by(visitor, offset):
    rings = lax.axis_size("blk") // RING
    within = offset % RING
    whole = (offset // RING + jnp.where(within > RING // 2, 1, 0)) % rings

    def mover(steps, pieces=1):
        def move(v):
            cut = v.shape[0] // pieces
            parts = [shifted(v[i * cut : (i + 1) * cut], "blk", steps) for i in range(pieces)]
            return jnp.concatenate(parts) if pieces > 1 else parts[0]

        return move if steps else (lambda v: v)

    visitor = lax.switch(whole, [mover(RING * j) for j in range(rings)], visitor)
    near = [j if j < 5 else j - RING if j > 7 else 0 for j in range(RING)]
    return lax.switch(within, [mover(j, 2 if abs(j) < 4 else 1) for j in near], visitor)


def paired(value, even, odd):
    count = lax.axis_size("rep")
    pairs = [(i, (i + (odd if i % 2 else even)) % count) for i in range(count)]
    return lax.ppermute(value, "rep", pairs)


def merge_kernel(place, parts, other, kept, ahead_rows, far, back):
    core, chip, ahead, behind, across = (place[i] for i in range(5))
    for target, at in ((far, across), (back, behind), (kept, chip), (ahead_rows, ahead)):
        for o in range(parts.shape[0]):
            for x in range(parts.shape[3]):
                t = parts[o, at, core, x] + other[o, at, x].astype(jnp.float32)
                target[o, x] = t.astype(target.dtype)


def merge(place, parts, other):
    count, _, _, rows = parts.shape[:4]
    shape = (count, rows, NY, NZ)
    kinds = (jnp.float32, jnp.float32, jnp.bfloat16, jnp.bfloat16)
    space = pl.BlockSpec(memory_space=pltpu.VMEM)
    return pl.pallas_call(
        merge_kernel,
        out_shape=[jax.ShapeDtypeStruct(shape, kind) for kind in kinds],
        grid_spec=pltpu.PrefetchScalarGridSpec(
            num_scalar_prefetch=1, grid=(), in_specs=[space] * 2, out_specs=[space] * 4
        ),
        compiler_params=pltpu.CompilerParams(vmem_limit_bytes=16 * 2**20),
        name="merge",
    )(place, parts, other)


def spread(field_sum):
    replica = lax.axis_index("rep")
    chips = lax.axis_size("rep") // 2
    core, chip = replica % 2, replica // 2
    ahead = jnp.where(core == 0, chip + 1, chip + chips - 1) % chips
    across = (chip + 2) % chips
    behind = (ahead + 2) % chips
    count = field_sum.shape[0]
    parts = field_sum.reshape(count, chips, 2, NX // (2 * chips), NY, NZ)
    sent = lax.dynamic_index_in_dim(parts, 1 - core, 2, keepdims=False).astype(jnp.bfloat16)
    other = paired(sent, 1, -1)
    place = jnp.stack([core, chip, ahead, behind, across]).astype(jnp.int32)
    kept, ahead_rows, far, back = merge(place, parts, other)
    far = paired(far, 2, -2)
    back = paired(back, -2, 2)
    near = paired((ahead_rows + far.astype(jnp.float32)).astype(jnp.bfloat16), 2, -2)
    return kept + back.astype(jnp.float32) + near.astype(jnp.float32)


def moved(visitor, target):
    owners = lax.axis_size("blk")
    steps = [target(b % RING) for b in range(owners)]
    return lax.ppermute(
        visitor, "blk", [(b, (b + n) % owners) for b, n in enumerate(steps) if n]
    )


def hop(visitor, way):
    return moved(visitor, lambda z: way if 0 <= z + way < RING else 0)


def carry(visitor, way, hops):
    start = RING - hops if way > 0 else hops - 1
    return moved(visitor, lambda z: way * hops if z == start else 0)


def chain(way, orbitals, constants, visitor):
    edge = lax.axis_index("blk") % RING == (0 if way > 0 else RING - 1)
    carried = [carry(visitor, way, hops) for hops in range(1, HOPS)]
    field_sum = None
    for hop_index in range(HOPS):
        following = None
        if hop_index < HOPS - 1:
            following = jnp.where(edge, carried[hop_index], hop(visitor, way))
        if following is None:
            return field_sum, visitor
        field_sum = add_pairs(orbitals, visitor, field_sum, constants)
        visitor = following


def span(offset):
    return jnp.minimum(offset % RING, RING - offset % RING)


def body(orbitals, skew):
    constants = lax.optimization_barrier(tables())
    replica = lax.axis_index("rep")
    start_orb = lax.dynamic_index_in_dim(orbitals, replica % orbitals.shape[0], 0, keepdims=False)
    last = skew[0] + HOPS - 1
    backward = span(last) < span(skew[0])
    first = jnp.where(backward, last, skew[0])
    visitor = shift_by(start_orb, first % lax.axis_size("blk"))
    field_sum, visitor = lax.cond(
        backward,
        functools.partial(chain, -1),
        functools.partial(chain, 1),
        orbitals,
        constants,
        visitor,
    )
    return spread(add_pairs(orbitals, visitor, field_sum, constants))


def solution(mesh):
    placed = (P("blk", None, None, None), P("rep"))
    return jax.shard_map(
        body, mesh=mesh, in_specs=placed, out_specs=P("blk", "rep", None, None), check_vma=False
    )
```
